32 devices in a mesh: rows: 2 (over core), cols: 2 (over y), slabs: 2 (over x), site: 4 (over z).
Axes of the slice: x: 2, y: 2, z: 4, core: 2. Of those that a mesh axis runs over, the one named last changes fastest.
Arguments:
- field_values: float32 [768, 16, 16, 128], P(('site', 'rows'), 'cols', 'slabs'), parts along dimension 0, may hold values from 0.5 to 2
- crowding: float32 [768, 16, 16, 128], P(('site', 'rows'), 'cols', 'slabs'), parts along dimension 0, may hold values from 0.5 to 2
Outputs:
- standardized: float32 [768, 16, 16, 128], P(('site', 'rows'), 'cols', 'slabs'), parts along dimension 0
- field_values_end: float32 [768, 16, 16, 128], P(('site', 'rows'), 'cols', 'slabs'), parts along dimension 0
The draws below stay inside these ranges and needn't reach their ends.
There are 4 independent parts, one for each index of `site`. The reference program is written for one: setup_inputs(seed, part) draws one part's arguments, and reference() takes and returns one part's arrays. A program takes and returns all parts, laid end to end along the dimension named above; each array names one. Nothing has to cross between parts.
All inputs are finite; a program needn't handle non-finite values.
Results may differ from the reference program's by a relative error of at most 0.000036.
Values sent between devices are 32-bit elements; how exact they have to be, the bound alone decides.
A program may use at most 64 MiB of HBM per device.

```python
import jax
import jax.numpy as jnp
from jax import lax

GRID_Y = 192
GRID_X = 16
GRID_Z = 16
LEVELS = 128
STEPS = 6


def levels(own_key, extent, cuts, low, top_value):
    gain, own = 1.0, jax.random.fold_in(own_key, 6)
    for axis_at, shards_of in cuts:
        draws = jnp.exp(jax.random.uniform(jax.random.fold_in(own, axis_at), (shards_of,), jnp.float32, low / len(cuts), top_value / len(cuts)))
        gain = gain * jnp.repeat(draws, extent[axis_at] // shards_of).reshape([-1 if axis == axis_at else 1 for axis in range(len(extent))])
    return gain


def setup_inputs(seed: int = 0, part: int = 0) -> dict:
    keys = jax.random.split(jax.random.key(seed), 3)
    part_splits = jax.random.split(jax.random.fold_in(keys[2], part), 3)
    field_values = jnp.clip(0.5 + 1.5 * jax.random.uniform(part_splits[0], (GRID_Y, GRID_X, GRID_Z, LEVELS), jnp.float32) ** levels(part_splits[0], (GRID_Y, GRID_X, GRID_Z, LEVELS), ((0, 2), (1, 2), (2, 2)), -0.2, 0.2), 0.5, 2.0)
    crowding = jnp.clip(0.5 + 1.5 * jax.random.uniform(part_splits[1], (GRID_Y, GRID_X, GRID_Z, LEVELS), jnp.float32) ** levels(part_splits[1], (GRID_Y, GRID_X, GRID_Z, LEVELS), ((0, 2), (1, 2), (2, 2)), -0.2, 0.2), 0.5, 2.0)
    return {"field_values": field_values, "crowding": crowding}


def inner_cells(values, dims):
    for dim in dims:
        values = lax.slice_in_dim(values, 1, values.shape[dim] - 1, axis=dim)
    return values

def side_cells(values, dim, start, dims):
    others = [other for other in dims if other != dim]
    values = inner_cells(values, others)
    return lax.slice_in_dim(values, start, start + values.shape[dim] - 2, axis=dim)

def advance(padded, crowding):
    middle = inner_cells(padded, (0, 1, 2))
    lower = [side_cells(padded, dim, 0, (0, 1, 2)) for dim in (0, 1, 2)]
    upper = [side_cells(padded, dim, 2, (0, 1, 2)) for dim in (0, 1, 2)]
    spread = lower[0] + upper[0] + lower[1] + upper[1] + lower[2] + upper[2] - 6.0 * middle
    return middle + 0.1 * spread + 0.2 * middle * (1.0 - middle * crowding)

def reference(field_values, crowding):
    for step in range(STEPS):
        field_values = advance(jnp.pad(field_values, ((1, 1), (1, 1), (1, 1), (0, 0)), mode='wrap'), crowding)
    line_mean = lax.optimization_barrier(jnp.mean(field_values, axis=0, keepdims=True))
    centred = field_values - line_mean
    line_variance = lax.optimization_barrier(jnp.mean(centred * centred, axis=0, keepdims=True))
    standardized = centred * lax.rsqrt(line_variance + 0.0001)
    return (standardized, field_values)
```

```python
import functools

import jax
import jax.numpy as jnp
from jax import lax
from jax.experimental import pallas as pl
from jax.experimental.pallas import tpu as pltpu
from jax.sharding import PartitionSpec as P

MESH = pl.DeviceIdType.MESH
STEPS = 6


def ring(axis, devices):
    me = lax.axis_index(axis)
    return lax.rem(me + 1, devices), lax.rem(me + devices - 1, devices)


def kernel(dims, f_hbm, c_hbm, end, moments, fbuf, cbuf, xsend, xrecv, zsend, zrecv,
           load_sem, crowd_sem, face_send, face_recv, row_send, row_recv, mom_send, mom_recv):
    rows, cols, slabs, size_y, size_x, size_z, chunks = dims
    ny = size_y // chunks
    levels = f_hbm.shape[-1]
    x_next = ring("cols", cols)
    z_next = ring("slabs", slabs)
    x_copies = 1 if cols == 2 else 2
    y_next = ring("rows", rows)
    tile = [pl.ds(x * size_z, size_z) for x in range(size_x)]

    def inner(j):
        return pl.ds(j * ny + 1, ny)

    def outer(j):
        return pl.ds(j * ny, ny)

    def faces(k, j):
        copies = []
        for at, (axis, devices, source, target, peers) in enumerate((
                ("cols", cols, xsend, xrecv, x_next), ("slabs", slabs, zsend, zrecv, z_next))):
            for side in range(1 if devices == 2 else 2):
                sides = pl.ds(side, 2 if devices == 2 else 1)
                copies.append(pltpu.make_async_remote_copy(
                    src_ref=source.at[k, sides, outer(j)], dst_ref=target.at[k, sides, outer(j)],
                    send_sem=face_send.at[k, j, 2 * at + side], recv_sem=face_recv.at[k, j, 2 * at + side],
                    device_id={axis: peers[side]}, device_id_type=MESH))
        return copies

    def y_copy(k, side):
        return pltpu.make_async_remote_copy(
            src_ref=fbuf.at[k, size_y if side == 0 else 1],
            dst_ref=fbuf.at[k, 0 if side == 0 else size_y + 1],
            send_sem=row_send.at[k, side], recv_sem=row_recv.at[k, side],
            device_id={"rows": y_next[side]}, device_id_type=MESH)

    def load(j):
        return pltpu.make_async_copy(f_hbm.at[outer(j)], fbuf.at[0, inner(j)], load_sem.at[j])

    def load_face(side):
        return pltpu.make_async_copy(
            f_hbm.at[:, tile[size_x - 1 if side == 0 else 0]], xsend.at[0, side], load_sem.at[chunks + side])

    crowd = pltpu.make_async_copy(c_hbm, cbuf, crowd_sem)

    def moment_copy(r):
        return pltpu.make_async_remote_copy(
            src_ref=moments.at[0], dst_ref=moments.at[r],
            send_sem=mom_send.at[r], recv_sem=mom_recv.at[r],
            device_id={"rows": lax.rem(lax.axis_index("rows") + r, rows)}, device_id_type=MESH)

    def start_faces(k, j):
        copies = faces(k, j)
        for copy in copies[:x_copies]:
            copy.start()

        @pl.when(j == 0)
        def _():
            y_copy(k, 1).start()

        @pl.when(j == chunks - 1)
        def _():
            y_copy(k, 0).start()

        @pl.loop(0, ny)
        def _(r):
            y = j * ny + r
            for side in (0, 1):
                first = size_z - 1 if side == 0 else 0
                zsend[k, side, y] = fbuf[k, y + 1, pl.ds(first, size_x, stride=size_z), :]

        for copy in copies[x_copies:]:
            copy.start()

    def wait_faces(k, j, recv):
        for copy in faces(k, j):
            if recv:
                copy.wait_recv()
            else:
                copy.wait_send()

        for side, at in ((0, 0 if recv else chunks - 1), (1, chunks - 1 if recv else 0)):
            @pl.when(j == at)
            def _():
                if recv:
                    y_copy(k, side).wait_recv()
                else:
                    y_copy(k, side).wait_send()

    at_z = lax.broadcasted_iota(jnp.int32, (size_z, levels), 0)

    def advance(k, j, sums):
        def row(r, sums):
            y = j * ny + r
            mid = [fbuf[k, y + 1, tile[x], :] for x in range(size_x)]
            out = []
            for x in range(size_x):
                m = mid[x]
                below = mid[x - 1] if x > 0 else xrecv[k, 0, y]
                above = mid[x + 1] if x < size_x - 1 else xrecv[k, 1, y]
                z_lo = jnp.broadcast_to(zrecv[k, 0, y, pl.ds(x, 1), :], m.shape)
                z_hi = jnp.broadcast_to(zrecv[k, 1, y, pl.ds(x, 1), :], m.shape)
                left = jnp.where(at_z == 0, z_lo, pltpu.roll(m, 1, 0))
                right = jnp.where(at_z == size_z - 1, z_hi, pltpu.roll(m, size_z - 1, 0))
                near = (fbuf[k, y, tile[x], :] + fbuf[k, y + 2, tile[x], :]) + (below + above) + (left + right)
                new = 0.1 * near + m * (0.6 - 0.2 * (m * cbuf[y, tile[x], :]))
                if sums:
                    end[y, tile[x], :] = new
                else:
                    fbuf[k + 1, y + 1, tile[x], :] = new
                    if x == size_x - 1:
                        xsend[k + 1, 0, y] = new
                    if x == 0:
                        xsend[k + 1, 1, y] = new
                out.append(new)
            return tuple(s + o for s, o in zip(sums, out)) if sums else ()

        return lax.fori_loop(0, ny, row, sums)

    load(0).start()
    for side in (0, 1):
        load_face(side).start()

    barrier = pltpu.get_barrier_semaphore()
    count = 0
    for axis, devices, peers in (("cols", cols, x_next), ("slabs", slabs, z_next)):
        for peer in peers[:1 if devices == 2 else 2]:
            pl.semaphore_signal(barrier, inc=1, device_id={axis: peer}, device_id_type=MESH)
            count += 1
    for r in range(1, rows):
        pl.semaphore_signal(barrier, inc=1, device_id={"rows": lax.rem(lax.axis_index("rows") + r, rows)}, device_id_type=MESH)
        count += 1
    pl.semaphore_wait(barrier, count)

    for j in range(1, chunks):
        load(j).start()
    for side in (0, 1):
        load_face(side).wait()

    @pl.loop(0, chunks)
    def _(j):
        load(j).wait()
        start_faces(0, j)

    crowd.start()
    crowd.wait()
    moments[0] = jnp.zeros(moments.shape[1:], jnp.float32)

    @pl.loop(0, STEPS - 1)
    def _(k):
        @pl.loop(0, chunks)
        def _(i):
            j = lax.rem(k + i, chunks)
            wait_faces(k, j, True)
            advance(k, j, ())
            start_faces(k + 1, j)
            wait_faces(k, j, False)

    last = STEPS - 1
    zero = jnp.zeros((size_z, levels), jnp.float32)

    @pl.loop(0, chunks)
    def _(i):
        j = lax.rem(last - 1 + i, chunks)
        wait_faces(last, j, True)
        sums = advance(last, j, (zero,) * size_x)
        means = tuple(s * (1.0 / ny) for s in sums)

        def spread(r, squares):
            deltas = [end[j * ny + r, tile[x], :] - means[x] for x in range(size_x)]
            return tuple(s + d * d for s, d in zip(squares, deltas))

        squares = lax.fori_loop(0, ny, spread, (zero,) * size_x)
        share = 1.0 / (i + 1).astype(jnp.float32)
        weight = i.astype(jnp.float32) * share * ny
        for x in range(size_x):
            delta = means[x] - moments[0, 0, tile[x], :]
            moments[0, 0, tile[x], :] += delta * share
            moments[0, 1, tile[x], :] += squares[x] + delta * delta * weight

    for r in range(1, rows):
        moment_copy(r).start()
    for r in range(1, rows):
        moment_copy(r).wait_recv()
    for r in range(1, rows):
        moment_copy(r).wait_send()

    @pl.loop(0, chunks)
    def _(j):
        wait_faces(last, j, False)


def finish(size_y, end, moments, standardized_hbm, end_hbm, out, end_sem, out_sem):
    rows = moments.shape[0]
    pieces = out_sem.shape[0]
    ny = size_y // pieces
    copy_end = pltpu.make_async_copy(end, end_hbm, end_sem)
    copy_end.start()

    parts = [moments[r, 0] for r in range(rows)]
    mean = sum(parts[1:], parts[0]) * (1.0 / rows)
    square = sum([moments[r, 1] for r in range(1, rows)], moments[0, 1])
    for p in parts:
        square = square + size_y * ((p - mean) * (p - mean))
    scale = lax.rsqrt(square * (1.0 / (rows * size_y)) + 0.0001)

    def store(j):
        return pltpu.make_async_copy(out.at[pl.ds(j * ny, ny)], standardized_hbm.at[pl.ds(j * ny, ny)], out_sem.at[j])

    for j in range(pieces):
        @pl.loop(0, ny)
        def _(r):
            y = j * ny + r
            out[y] = (end[y] - mean) * scale

        store(j).start()

    for j in range(pieces):
        store(j).wait()
    copy_end.wait()


def local(dims, field_values, crowding):
    shape = field_values.shape
    size_y, size_x, size_z, levels = shape
    rows, cols, slabs = dims
    chunks = next(n for n in (4, 3, 6, 2, 1) if size_y % n == 0)
    flat = (size_y, size_x * size_z, levels)
    dma = pltpu.SemaphoreType.DMA
    held = (flat, (rows, 2) + flat[1:])
    out = tuple(pltpu.VMEM(each, jnp.float32) for each in held)
    vmem_spec = pl.BlockSpec(memory_space=pltpu.VMEM)
    any_spec = pl.BlockSpec(memory_space=pl.ANY)
    field_end, moments = pl.pallas_call(
        functools.partial(kernel, (rows, cols, slabs, size_y, size_x, size_z, chunks)),
        out_shape=out,
        in_specs=[any_spec] * 2,
        out_specs=(vmem_spec,) * 2,
        scratch_shapes=[
            pltpu.VMEM((STEPS, size_y + 2, size_x * size_z, levels), jnp.float32),
            pltpu.VMEM(flat, jnp.float32),
            pltpu.VMEM((STEPS, 2, size_y, size_z, levels), jnp.float32),
            pltpu.VMEM((STEPS, 2, size_y, size_z, levels), jnp.float32),
            pltpu.VMEM((STEPS, 2, size_y, size_x, levels), jnp.float32),
            pltpu.VMEM((STEPS, 2, size_y, size_x, levels), jnp.float32),
            dma((chunks + 2,)),
            dma,
            dma((STEPS, chunks, 4)),
            dma((STEPS, chunks, 4)),
            dma((STEPS, 2)),
            dma((STEPS, 2)),
            dma((rows,)),
            dma((rows,)),
        ],
        compiler_params=pltpu.CompilerParams(
            collective_id=0, has_side_effects=True, vmem_limit_bytes=58 * 1024 * 1024),
    )(field_values.reshape(flat), crowding.reshape(flat))
    whole = jax.ShapeDtypeStruct(flat, jnp.float32)
    standardized, field_end = pl.pallas_call(
        functools.partial(finish, size_y),
        out_shape=(whole, whole),
        in_specs=[vmem_spec] * 2,
        out_specs=(any_spec,) * 2,
        scratch_shapes=[pltpu.VMEM(flat, jnp.float32), dma, dma((chunks,))],
        compiler_params=pltpu.CompilerParams(vmem_limit_bytes=16 * 1024 * 1024),
    )(*(pltpu.with_memory_space_constraint(each, pltpu.VMEM) for each in (field_end, moments)))
    return standardized.reshape(shape), field_end.reshape(shape)


def solution(mesh):
    spec = P(("site", "rows"), "cols", "slabs", None)
    dims = tuple(mesh.shape[axis] for axis in ("rows", "cols", "slabs"))
    return jax.shard_map(
        functools.partial(local, dims), mesh=mesh,
        in_specs=(spec, spec), out_specs=(spec, spec), check_vma=False)
```

```python
import functools

import jax
import jax.numpy as jnp
from jax import lax
from jax.experimental import pallas as pl
from jax.experimental.pallas import tpu as pltpu
from jax.sharding import PartitionSpec as P

MESH = pl.DeviceIdType.MESH
STEPS = 6


def ring(axis, devices):
    me = lax.axis_index(axis)
    return lax.rem(me + 1, devices), lax.rem(me + devices - 1, devices)


def pieces_of(size_y):
    small = max(1, size_y // 12)

    def cut(*ends):
        ends = sorted({e for e in ends if 0 < e < size_y} | {0, size_y})
        return tuple((lo, hi - lo) for lo, hi in zip(ends, ends[1:]))

    middle = tuple(size_y * i // 2 for i in range(1, 2))
    first = cut(small, *middle)
    last = cut(size_y - small, *middle)
    return (first,) + (cut(*middle),) * (STEPS - 2) + (last,)


def kernel(dims, f_hbm, c_hbm, end, moments, fbuf, cbuf, xsend, xrecv, zsend, zrecv,
           load_sem, crowd_sem, face_send, face_recv, row_send, row_recv, mom_send, mom_recv):
    rows, cols, slabs, size_y, size_x, size_z = dims
    pieces = pieces_of(size_y)
    levels = f_hbm.shape[-1]
    x_next = ring("cols", cols)
    z_next = ring("slabs", slabs)
    x_copies = 1 if cols == 2 else 2
    y_next = ring("rows", rows)
    tile = [pl.ds(x * size_z, size_z) for x in range(size_x)]

    def faces(k, p):
        copies = []
        at_rows = pl.ds(*pieces[k][p])
        for axis, devices, source, target, peers in (
                ("cols", cols, xsend, xrecv, x_next), ("slabs", slabs, zsend, zrecv, z_next)):
            for side in range(1 if devices == 2 else 2):
                sides = pl.ds(side, 2 if devices == 2 else 1)
                copies.append(pltpu.make_async_remote_copy(
                    src_ref=source.at[k, sides, at_rows], dst_ref=target.at[k, sides, at_rows],
                    send_sem=face_send.at[len(copies)], recv_sem=face_recv.at[k % 2, p, len(copies)],
                    device_id={axis: peers[side]}, device_id_type=MESH))
        return copies

    def y_copy(k, side):
        return pltpu.make_async_remote_copy(
            src_ref=fbuf.at[k, size_y if side == 0 else 1],
            dst_ref=fbuf.at[k, 0 if side == 0 else size_y + 1],
            send_sem=row_send, recv_sem=row_recv.at[k % 2, side],
            device_id={"rows": y_next[side]}, device_id_type=MESH)

    def load(p):
        lo, ny = pieces[0][p]
        return pltpu.make_async_copy(f_hbm.at[pl.ds(lo, ny)], fbuf.at[0, pl.ds(lo + 1, ny)], load_sem.at[p])

    crowd = pltpu.make_async_copy(c_hbm, cbuf, crowd_sem)

    def moment_copy(r):
        return pltpu.make_async_remote_copy(
            src_ref=moments.at[0], dst_ref=moments.at[r],
            send_sem=mom_send.at[r - 1], recv_sem=mom_recv.at[r - 1],
            device_id={"rows": lax.rem(lax.axis_index("rows") + r, rows)}, device_id_type=MESH)

    def start_faces(k, p):
        lo, ny = pieces[k][p]
        copies = faces(k, p)
        if k:
            for copy in copies[:x_copies]:
                copy.start()

        @pl.loop(0, ny)
        def _(r):
            y = lo + r
            for side in (0, 1):
                first = size_z - 1 if side == 0 else 0
                zsend[k, side, y] = fbuf[k, y + 1, pl.ds(first, size_x, stride=size_z), :]
                if not k:
                    xsend[k, side, y] = fbuf[k, y + 1, tile[size_x - 1 if side == 0 else 0], :]

        for copy in copies[x_copies if k else 0:]:
            copy.start()

    def start_y(k, p):
        lo, ny = pieces[k][p]
        if lo == 0:
            y_copy(k, 1).start()
        if lo + ny == size_y:
            y_copy(k, 0).start()

    def wait_recv(k, p):
        lo, ny = pieces[k][p]
        for copy in faces(k, p):
            copy.wait_recv()
        if lo == 0:
            y_copy(k, 0).wait_recv()
        if lo + ny == size_y:
            y_copy(k, 1).wait_recv()

    at_z = lax.broadcasted_iota(jnp.int32, (size_z, levels), 0)

    def advance(k, p, sums):
        lo, ny = pieces[k][p]

        def row(r, sums):
            y = lo + r
            mid = [fbuf[k, y + 1, tile[x], :] for x in range(size_x)]
            out = []
            for x in range(size_x):
                m = mid[x]
                below = mid[x - 1] if x > 0 else xrecv[k, 0, y]
                above = mid[x + 1] if x < size_x - 1 else xrecv[k, 1, y]
                z_lo = jnp.broadcast_to(zrecv[k, 0, y, pl.ds(x, 1), :], m.shape)
                z_hi = jnp.broadcast_to(zrecv[k, 1, y, pl.ds(x, 1), :], m.shape)
                left = jnp.where(at_z == 0, z_lo, pltpu.roll(m, 1, 0))
                right = jnp.where(at_z == size_z - 1, z_hi, pltpu.roll(m, size_z - 1, 0))
                near = (fbuf[k, y, tile[x], :] + fbuf[k, y + 2, tile[x], :]) + (below + above) + (left + right)
                new = 0.1 * near + m * (0.6 - 0.2 * (m * cbuf[y, tile[x], :]))
                if sums:
                    end[y, tile[x], :] = new
                else:
                    fbuf[k + 1, y + 1, tile[x], :] = new
                    if x == size_x - 1:
                        xsend[k + 1, 0, y] = new
                    if x == 0:
                        xsend[k + 1, 1, y] = new
                out.append(new)
            return tuple(s + o for s, o in zip(sums, out)) if sums else ()

        return lax.fori_loop(0, ny, row, sums)

    load(0).start()

    barrier = pltpu.get_barrier_semaphore()
    count = 0
    for axis, devices, peers in (("cols", cols, x_next), ("slabs", slabs, z_next)):
        for peer in peers[:1 if devices == 2 else 2]:
            pl.semaphore_signal(barrier, inc=1, device_id={axis: peer}, device_id_type=MESH)
            count += 1
    for r in range(1, rows):
        pl.semaphore_signal(barrier, inc=1, device_id={"rows": lax.rem(lax.axis_index("rows") + r, rows)}, device_id_type=MESH)
        count += 1

    load(1).start()
    pl.semaphore_wait(barrier, count)

    for p in range(len(pieces[0])):
        if p + 2 < len(pieces[0]):
            load(p + 2).start()
        load(p).wait()
        start_faces(0, p)
        start_y(0, p)
    crowd.start()
    crowd.wait()

    last = STEPS - 1
    for k in range(last):
        sent, ready = set(), 0
        for p, (lo, ny) in enumerate(pieces[k]):
            wait_recv(k, p)
            advance(k, p, ())
            ready = lo + ny
            for q, (q_lo, q_ny) in enumerate(pieces[k + 1]):
                if q not in sent and q_lo + q_ny <= ready:
                    sent.add(q)
                    start_faces(k + 1, q)
                    start_y(k + 1, q)

    zero = jnp.zeros((size_z, levels), jnp.float32)
    done = 0
    for p, (lo, ny) in enumerate(pieces[last]):
        wait_recv(last, p)
        sums = advance(last, p, (zero,) * size_x)
        means = tuple(s * (1.0 / ny) for s in sums)

        def spread(r, squares):
            deltas = [end[lo + r, tile[x], :] - means[x] for x in range(size_x)]
            return tuple(s + d * d for s, d in zip(squares, deltas))

        squares = lax.fori_loop(0, ny, spread, (zero,) * size_x)
        share = ny / (done + ny)
        for x in range(size_x):
            if done == 0:
                moments[0, 0, tile[x], :] = means[x]
                moments[0, 1, tile[x], :] = squares[x]
            else:
                delta = means[x] - moments[0, 0, tile[x], :]
                moments[0, 0, tile[x], :] += delta * share
                moments[0, 1, tile[x], :] += squares[x] + delta * delta * (done * share)
        done += ny

    for r in range(1, rows):
        moment_copy(r).start()
    at = 0
    for devices, source in ((cols, xsend), (slabs, zsend)):
        for side in range(1 if devices == 2 else 2):
            sides = pl.ds(side, 2 if devices == 2 else 1)
            sent = source.at[:, sides]
            pltpu.make_async_copy(sent, sent, face_send.at[at]).wait()
            at += 1
    sent = fbuf.at[0, pl.ds(0, 2 * STEPS)]
    pltpu.make_async_copy(sent, sent, row_send).wait()
    for r in range(1, rows):
        moment_copy(r).wait()


def finish(size_y, pieces, end, moments, standardized_hbm, end_hbm, out, end_sem, out_sem):
    rows = moments.shape[0]
    ny = size_y // pieces
    copy_end = pltpu.make_async_copy(end, end_hbm, end_sem)
    copy_end.start()

    parts = [moments[r, 0] for r in range(rows)]
    mean = sum(parts[1:], parts[0]) * (1.0 / rows)
    square = sum([moments[r, 1] for r in range(1, rows)], moments[0, 1])
    for p in parts:
        square = square + size_y * ((p - mean) * (p - mean))
    scale = lax.rsqrt(square * (1.0 / (rows * size_y)) + 0.0001)

    def store(j):
        return pltpu.make_async_copy(out.at[pl.ds(j * ny, ny)], standardized_hbm.at[pl.ds(j * ny, ny)], out_sem)

    for j in range(pieces):
        @pl.loop(0, ny)
        def _(r):
            y = j * ny + r
            out[y] = (end[y] - mean) * scale

        store(j).start()

    pltpu.make_async_copy(out, standardized_hbm, out_sem).wait()
    copy_end.wait()


def local(dims, field_values, crowding):
    shape = field_values.shape
    size_y, size_x, size_z, levels = shape
    rows, cols, slabs = dims
    most = max(map(len, pieces_of(size_y)))
    links = sum(1 if devices == 2 else 2 for devices in (cols, slabs))
    chunks = next(n for n in (4, 3, 6, 2, 1) if size_y % n == 0)
    flat = (size_y, size_x * size_z, levels)
    dma = pltpu.SemaphoreType.DMA
    held = (flat, (rows, 2) + flat[1:])
    out = tuple(pltpu.VMEM(each, jnp.float32) for each in held)
    vmem_spec = pl.BlockSpec(memory_space=pltpu.VMEM)
    any_spec = pl.BlockSpec(memory_space=pl.ANY)
    field_end, moments = pl.pallas_call(
        functools.partial(kernel, (rows, cols, slabs, size_y, size_x, size_z)),
        out_shape=out,
        in_specs=[any_spec] * 2,
        out_specs=(vmem_spec,) * 2,
        scratch_shapes=[
            pltpu.VMEM((STEPS, size_y + 2, size_x * size_z, levels), jnp.float32),
            pltpu.VMEM(flat, jnp.float32),
            pltpu.VMEM((STEPS, 2, size_y, size_z, levels), jnp.float32),
            pltpu.VMEM((STEPS, 2, size_y, size_z, levels), jnp.float32),
            pltpu.VMEM((STEPS, 2, size_y, size_x, levels), jnp.float32),
            pltpu.VMEM((STEPS, 2, size_y, size_x, levels), jnp.float32),
            dma((len(pieces_of(size_y)[0]),)),
            dma,
            dma((links,)),
            dma((2, most, links)),
            dma,
            dma((2, 2)),
            dma((rows - 1,)),
            dma((rows - 1,)),
        ],
        compiler_params=pltpu.CompilerParams(
            collective_id=0, has_side_effects=True, vmem_limit_bytes=58 * 1024 * 1024),
    )(field_values.reshape(flat), crowding.reshape(flat))
    whole = jax.ShapeDtypeStruct(flat, jnp.float32)
    standardized, field_end = pl.pallas_call(
        functools.partial(finish, size_y, chunks),
        out_shape=(whole, whole),
        in_specs=[vmem_spec] * 2,
        out_specs=(any_spec,) * 2,
        scratch_shapes=[pltpu.VMEM(flat, jnp.float32), dma, dma],
        compiler_params=pltpu.CompilerParams(vmem_limit_bytes=16 * 1024 * 1024),
    )(*(pltpu.with_memory_space_constraint(each, pltpu.VMEM) for each in (field_end, moments)))
    return standardized.reshape(shape), field_end.reshape(shape)


def solution(mesh):
    spec = P(("site", "rows"), "cols", "slabs", None)
    dims = tuple(mesh.shape[axis] for axis in ("rows", "cols", "slabs"))
    return jax.shard_map(
        functools.partial(local, dims), mesh=mesh,
        in_specs=(spec, spec), out_specs=(spec, spec), check_vma=False)
```

```python
import functools

import jax
import jax.numpy as jnp
from jax import lax
from jax.experimental import pallas as pl
from jax.experimental.pallas import tpu as pltpu
from jax.sharding import PartitionSpec as P

MESH = pl.DeviceIdType.MESH
STEPS = 6


def ring(axis, devices):
    me = lax.axis_index(axis)
    return lax.rem(me + 1, devices), lax.rem(me + devices - 1, devices)


def pieces_of(size_y):
    def cut(*parts):
        ends = sorted({size_y * part // 24 for part in parts} | {0, size_y})
        return tuple((lo, hi - lo) for lo, hi in zip(ends, ends[1:]))

    return (cut(2, 8, 16),) + (cut(8, 16),) * (STEPS - 2) + (cut(10, 17, 21, 23),)


def kernel(dims, f_hbm, c_hbm, end, moments, fbuf, cbuf, xsend, xrecv, zsend, zrecv,
           load_sem, crowd_sem, face_send, face_recv, row_send, row_recv, mom_send, mom_recv):
    rows, cols, slabs, size_y, size_x, size_z = dims
    pieces = pieces_of(size_y)
    levels = f_hbm.shape[-1]
    x_next = ring("cols", cols)
    z_next = ring("slabs", slabs)
    x_copies = 1 if cols == 2 else 2
    y_next = ring("rows", rows)
    tile = [pl.ds(x * size_z, size_z) for x in range(size_x)]

    def faces(k, p):
        copies = []
        at_rows = pl.ds(*pieces[k][p])
        for axis, devices, source, target, peers in (
                ("cols", cols, xsend, xrecv, x_next), ("slabs", slabs, zsend, zrecv, z_next)):
            for side in range(1 if devices == 2 else 2):
                sides = pl.ds(side, 2 if devices == 2 else 1)
                copies.append(pltpu.make_async_remote_copy(
                    src_ref=source.at[k, sides, at_rows], dst_ref=target.at[k, sides, at_rows],
                    send_sem=face_send.at[len(copies)], recv_sem=face_recv.at[k % 2, p, len(copies)],
                    device_id={axis: peers[side]}, device_id_type=MESH))
        return copies

    def y_copy(k, side):
        return pltpu.make_async_remote_copy(
            src_ref=fbuf.at[k, size_y if side == 0 else 1],
            dst_ref=fbuf.at[k, 0 if side == 0 else size_y + 1],
            send_sem=row_send, recv_sem=row_recv.at[k % 2, side],
            device_id={"rows": y_next[side]}, device_id_type=MESH)

    def load(p):
        lo, ny = pieces[0][p]
        return pltpu.make_async_copy(f_hbm.at[pl.ds(lo, ny)], fbuf.at[0, pl.ds(lo + 1, ny)], load_sem.at[p])

    crowd = pltpu.make_async_copy(c_hbm, cbuf, crowd_sem)

    def moment_copy(r):
        return pltpu.make_async_remote_copy(
            src_ref=moments.at[0], dst_ref=moments.at[r],
            send_sem=mom_send.at[r - 1], recv_sem=mom_recv.at[r - 1],
            device_id={"rows": lax.rem(lax.axis_index("rows") + r, rows)}, device_id_type=MESH)

    def start_faces(k, p):
        lo, ny = pieces[k][p]
        copies = faces(k, p)
        if k:
            for copy in copies[:x_copies]:
                copy.start()

        @pl.loop(0, ny)
        def _(r):
            y = lo + r
            for side in (0, 1):
                first = size_z - 1 if side == 0 else 0
                zsend[k, side, y] = fbuf[k, y + 1, pl.ds(first, size_x, stride=size_z), :]
                if not k:
                    xsend[k, side, y] = fbuf[k, y + 1, tile[size_x - 1 if side == 0 else 0], :]

        for copy in copies[x_copies if k else 0:]:
            copy.start()

    def start_y(k, p):
        lo, ny = pieces[k][p]
        if lo == 0:
            y_copy(k, 1).start()
        if lo + ny == size_y:
            y_copy(k, 0).start()

    def wait_recv(k, p):
        lo, ny = pieces[k][p]
        for copy in faces(k, p):
            copy.wait_recv()
        if lo == 0:
            y_copy(k, 0).wait_recv()
        if lo + ny == size_y:
            y_copy(k, 1).wait_recv()

    at_z = lax.broadcasted_iota(jnp.int32, (size_z, levels), 0)

    def advance(k, p, sums):
        lo, ny = pieces[k][p]

        def row(r, sums):
            y = lo + r
            mid = [fbuf[k, y + 1, tile[x], :] for x in range(size_x)]
            out = []
            for x in range(size_x):
                m = mid[x]
                below = mid[x - 1] if x > 0 else xrecv[k, 0, y]
                above = mid[x + 1] if x < size_x - 1 else xrecv[k, 1, y]
                z_lo = jnp.broadcast_to(zrecv[k, 0, y, pl.ds(x, 1), :], m.shape)
                z_hi = jnp.broadcast_to(zrecv[k, 1, y, pl.ds(x, 1), :], m.shape)
                left = jnp.where(at_z == 0, z_lo, pltpu.roll(m, 1, 0))
                right = jnp.where(at_z == size_z - 1, z_hi, pltpu.roll(m, size_z - 1, 0))
                near = (fbuf[k, y, tile[x], :] + fbuf[k, y + 2, tile[x], :]) + (below + above) + (left + right)
                new = 0.1 * near + m * (0.6 - 0.2 * (m * cbuf[y, tile[x], :]))
                if sums:
                    end[y, tile[x], :] = new
                else:
                    fbuf[k + 1, y + 1, tile[x], :] = new
                    if x == size_x - 1:
                        xsend[k + 1, 0, y] = new
                    if x == 0:
                        xsend[k + 1, 1, y] = new
                out.append(new)
            return tuple(s + o for s, o in zip(sums, out)) if sums else ()

        return lax.fori_loop(0, ny, row, sums)

    load(0).start()

    barrier = pltpu.get_barrier_semaphore()
    count = 0
    for axis, devices, peers in (("cols", cols, x_next), ("slabs", slabs, z_next)):
        for peer in peers[:1 if devices == 2 else 2]:
            pl.semaphore_signal(barrier, inc=1, device_id={axis: peer}, device_id_type=MESH)
            count += 1
    for r in range(1, rows):
        pl.semaphore_signal(barrier, inc=1, device_id={"rows": lax.rem(lax.axis_index("rows") + r, rows)}, device_id_type=MESH)
        count += 1

    load(1).start()
    pl.semaphore_wait(barrier, count)

    for p in range(len(pieces[0])):
        if p + 2 < len(pieces[0]):
            load(p + 2).start()
        load(p).wait()
        start_faces(0, p)
        start_y(0, p)
    crowd.start()
    crowd.wait()

    last = STEPS - 1
    for k in range(last):
        sent, ready = set(), 0
        for p, (lo, ny) in enumerate(pieces[k]):
            wait_recv(k, p)
            advance(k, p, ())
            ready = lo + ny
            for q, (q_lo, q_ny) in enumerate(pieces[k + 1]):
                if q not in sent and q_lo + q_ny <= ready:
                    sent.add(q)
                    start_faces(k + 1, q)
                    start_y(k + 1, q)

    zero = jnp.zeros((size_z, levels), jnp.float32)
    done = 0
    for p, (lo, ny) in enumerate(pieces[last]):
        wait_recv(last, p)
        sums = advance(last, p, (zero,) * size_x)
        means = tuple(s * (1.0 / ny) for s in sums)

        def spread(r, squares):
            deltas = [end[lo + r, tile[x], :] - means[x] for x in range(size_x)]
            return tuple(s + d * d for s, d in zip(squares, deltas))

        squares = lax.fori_loop(0, ny, spread, (zero,) * size_x)
        share = ny / (done + ny)
        for x in range(size_x):
            if done == 0:
                moments[0, 0, tile[x], :] = means[x]
                moments[0, 1, tile[x], :] = squares[x]
            else:
                delta = means[x] - moments[0, 0, tile[x], :]
                moments[0, 0, tile[x], :] += delta * share
                moments[0, 1, tile[x], :] += squares[x] + delta * delta * (done * share)
        done += ny

    for r in range(1, rows):
        moment_copy(r).start()
    at = 0
    for devices, source in ((cols, xsend), (slabs, zsend)):
        for side in range(1 if devices == 2 else 2):
            sides = pl.ds(side, 2 if devices == 2 else 1)
            sent = source.at[:, sides]
            pltpu.make_async_copy(sent, sent, face_send.at[at]).wait()
            at += 1
    sent = fbuf.at[0, pl.ds(0, 2 * STEPS)]
    pltpu.make_async_copy(sent, sent, row_send).wait()
    for r in range(1, rows):
        moment_copy(r).wait()


def finish(size_y, pieces, end, moments, standardized_hbm, end_hbm, out, end_sem, out_sem):
    rows = moments.shape[0]
    ny = size_y // pieces
    copy_end = pltpu.make_async_copy(end, end_hbm, end_sem)
    copy_end.start()

    parts = [moments[r, 0] for r in range(rows)]
    mean = sum(parts[1:], parts[0]) * (1.0 / rows)
    square = sum([moments[r, 1] for r in range(1, rows)], moments[0, 1])
    for p in parts:
        square = square + size_y * ((p - mean) * (p - mean))
    scale = lax.rsqrt(square * (1.0 / (rows * size_y)) + 0.0001)

    def store(j):
        return pltpu.make_async_copy(out.at[pl.ds(j * ny, ny)], standardized_hbm.at[pl.ds(j * ny, ny)], out_sem)

    for j in range(pieces):
        @pl.loop(0, ny)
        def _(r):
            y = j * ny + r
            out[y] = (end[y] - mean) * scale

        store(j).start()

    pltpu.make_async_copy(out, standardized_hbm, out_sem).wait()
    copy_end.wait()


def local(dims, field_values, crowding):
    shape = field_values.shape
    size_y, size_x, size_z, levels = shape
    rows, cols, slabs = dims
    most = max(map(len, pieces_of(size_y)))
    links = sum(1 if devices == 2 else 2 for devices in (cols, slabs))
    chunks = next(n for n in (4, 3, 6, 2, 1) if size_y % n == 0)
    flat = (size_y, size_x * size_z, levels)
    dma = pltpu.SemaphoreType.DMA
    held = (flat, (rows, 2) + flat[1:])
    out = tuple(pltpu.VMEM(each, jnp.float32) for each in held)
    vmem_spec = pl.BlockSpec(memory_space=pltpu.VMEM)
    any_spec = pl.BlockSpec(memory_space=pl.ANY)
    field_end, moments = pl.pallas_call(
        functools.partial(kernel, (rows, cols, slabs, size_y, size_x, size_z)),
        out_shape=out,
        in_specs=[any_spec] * 2,
        out_specs=(vmem_spec,) * 2,
        scratch_shapes=[
            pltpu.VMEM((STEPS, size_y + 2, size_x * size_z, levels), jnp.float32),
            pltpu.VMEM(flat, jnp.float32),
            pltpu.VMEM((STEPS, 2, size_y, size_z, levels), jnp.float32),
            pltpu.VMEM((STEPS, 2, size_y, size_z, levels), jnp.float32),
            pltpu.VMEM((STEPS, 2, size_y, size_x, levels), jnp.float32),
            pltpu.VMEM((STEPS, 2, size_y, size_x, levels), jnp.float32),
            dma((len(pieces_of(size_y)[0]),)),
            dma,
            dma((links,)),
            dma((2, most, links)),
            dma,
            dma((2, 2)),
            dma((rows - 1,)),
            dma((rows - 1,)),
        ],
        compiler_params=pltpu.CompilerParams(
            collective_id=0, has_side_effects=True, vmem_limit_bytes=58 * 1024 * 1024),
    )(field_values.reshape(flat), crowding.reshape(flat))
    whole = jax.ShapeDtypeStruct(flat, jnp.float32)
    standardized, field_end = pl.pallas_call(
        functools.partial(finish, size_y, chunks),
        out_shape=(whole, whole),
        in_specs=[vmem_spec] * 2,
        out_specs=(any_spec,) * 2,
        scratch_shapes=[pltpu.VMEM(flat, jnp.float32), dma, dma],
        compiler_params=pltpu.CompilerParams(vmem_limit_bytes=16 * 1024 * 1024),
    )(*(pltpu.with_memory_space_constraint(each, pltpu.VMEM) for each in (field_end, moments)))
    return standardized.reshape(shape), field_end.reshape(shape)


def solution(mesh):
    spec = P(("site", "rows"), "cols", "slabs", None)
    dims = tuple(mesh.shape[axis] for axis in ("rows", "cols", "slabs"))
    return jax.shard_map(
        functools.partial(local, dims), mesh=mesh,
        in_specs=(spec, spec), out_specs=(spec, spec), check_vma=False)
```

```python
import functools

import jax
import jax.numpy as jnp
from jax import lax
from jax.experimental import pallas as pl
from jax.experimental.pallas import tpu as pltpu
from jax.sharding import PartitionSpec as P

MESH = pl.DeviceIdType.MESH
STEPS = 6


def ring(axis, devices):
    me = lax.axis_index(axis)
    return lax.rem(me + 1, devices), lax.rem(me + devices - 1, devices)


def pieces_of(size_y):
    def cut(*parts):
        ends = sorted({size_y * part // 24 for part in parts} | {0, size_y})
        return tuple((lo, hi - lo) for lo, hi in zip(ends, ends[1:]))

    return (cut(2, 8, 16),) + (cut(8, 16),) * (STEPS - 2) + (cut(10, 17, 21, 23),)


def kernel(dims, f_hbm, c_hbm, end, moments, fbuf, cbuf, fsend, frecv,
           load_sem, face_send, face_recv, core_send, row_recv, mom_recv):
    rows, cols, slabs, size_y, size_x, size_z = dims
    pieces = pieces_of(size_y)
    common = min(map(len, pieces))
    levels = f_hbm.shape[-1]
    x_next = ring("cols", cols)
    z_next = ring("slabs", slabs)
    x_copies = 1 if cols == 2 else 2
    y_next = ring("rows", rows)
    tile = [pl.ds(x * size_z, size_z) for x in range(size_x)]

    x_part = [pl.ds(side * size_z, size_z) for side in (0, 1)]
    z_first = [2 * size_z + side * size_x for side in (0, 1)]
    z_part = [pl.ds(first, size_x) for first in z_first]

    def arrived(k, p):
        return (k % 2) * common + p if p < common else 2 * common + p - common

    def faces(k, p):
        copies = []
        at_rows = pl.ds(*pieces[k][p])
        for axis, devices, parts, whole, peers in (
                ("cols", cols, x_part, pl.ds(0, 2 * size_z), x_next),
                ("slabs", slabs, z_part, pl.ds(2 * size_z, 2 * size_x), z_next)):
            for side in range(1 if devices == 2 else 2):
                part = whole if devices == 2 else parts[side]
                copies.append(pltpu.make_async_remote_copy(
                    src_ref=fsend.at[k, at_rows, part], dst_ref=frecv.at[k, at_rows, part],
                    send_sem=face_send, recv_sem=face_recv.at[arrived(k, p)],
                    device_id={axis: peers[side]}, device_id_type=MESH))
        return copies

    def y_copy(k, side):
        return pltpu.make_async_remote_copy(
            src_ref=fbuf.at[k, size_y if side == 0 else 1],
            dst_ref=fbuf.at[k, 0 if side == 0 else size_y + 1],
            send_sem=core_send, recv_sem=row_recv.at[k % 2],
            device_id={"rows": y_next[side]}, device_id_type=MESH)

    def wait_bytes(ref, sem):
        pltpu.make_async_copy(ref, ref, sem).wait()

    def load(p):
        lo, ny = pieces[0][p]
        return pltpu.make_async_copy(f_hbm.at[pl.ds(lo, ny)], fbuf.at[0, pl.ds(lo + 1, ny)], load_sem.at[p % 2])

    crowd = pltpu.make_async_copy(c_hbm, cbuf, load_sem.at[0])

    def moment_copy(r):
        return pltpu.make_async_remote_copy(
            src_ref=moments.at[0], dst_ref=moments.at[r],
            send_sem=core_send, recv_sem=mom_recv.at[r - 1],
            device_id={"rows": lax.rem(lax.axis_index("rows") + r, rows)}, device_id_type=MESH)

    def start_faces(k, p):
        lo, ny = pieces[k][p]
        copies = faces(k, p)
        if k:
            for copy in copies[:x_copies]:
                copy.start()

        @pl.loop(0, ny)
        def _(r):
            y = lo + r
            for side in (0, 1):
                first = size_z - 1 if side == 0 else 0
                fsend[k, y, z_part[side]] = fbuf[k, y + 1, pl.ds(first, size_x, stride=size_z), :]
                if not k:
                    fsend[k, y, x_part[side]] = fbuf[k, y + 1, tile[size_x - 1 if side == 0 else 0], :]

        for copy in copies[x_copies if k else 0:]:
            copy.start()

    def start_y(k, p):
        lo, ny = pieces[k][p]
        if lo == 0:
            y_copy(k, 1).start()
        if lo + ny == size_y:
            y_copy(k, 0).start()

    def wait_recv(k, p):
        lo, ny = pieces[k][p]
        wait_bytes(frecv.at[k, pl.ds(lo, ny)], face_recv.at[arrived(k, p)])
        if p == 0:
            wait_bytes(fbuf.at[k, pl.ds(0, 2)], row_recv.at[k % 2])

    at_z = lax.broadcasted_iota(jnp.int32, (size_z, levels), 0)

    def advance(k, p, sums):
        lo, ny = pieces[k][p]

        def row(r, sums):
            y = lo + r
            mid = [fbuf[k, y + 1, tile[x], :] for x in range(size_x)]
            out = []
            for x in range(size_x):
                m = mid[x]
                below = mid[x - 1] if x > 0 else frecv[k, y, x_part[0]]
                above = mid[x + 1] if x < size_x - 1 else frecv[k, y, x_part[1]]
                z_lo = jnp.broadcast_to(frecv[k, y, pl.ds(z_first[0] + x, 1), :], m.shape)
                z_hi = jnp.broadcast_to(frecv[k, y, pl.ds(z_first[1] + x, 1), :], m.shape)
                left = jnp.where(at_z == 0, z_lo, pltpu.roll(m, 1, 0))
                right = jnp.where(at_z == size_z - 1, z_hi, pltpu.roll(m, size_z - 1, 0))
                near = (fbuf[k, y, tile[x], :] + fbuf[k, y + 2, tile[x], :]) + (below + above) + (left + right)
                new = 0.1 * near + m * (0.6 - 0.2 * (m * cbuf[y, tile[x], :]))
                if sums:
                    end[y, tile[x], :] = new
                else:
                    fbuf[k + 1, y + 1, tile[x], :] = new
                    if x == size_x - 1:
                        fsend[k + 1, y, x_part[0]] = new
                    if x == 0:
                        fsend[k + 1, y, x_part[1]] = new
                out.append(new)
            return tuple(s + o for s, o in zip(sums, out)) if sums else ()

        return lax.fori_loop(0, ny, row, sums)

    load(0).start()

    barrier = pltpu.get_barrier_semaphore()
    count = 0
    for axis, devices, peers in (("cols", cols, x_next), ("slabs", slabs, z_next)):
        for peer in peers[:1 if devices == 2 else 2]:
            pl.semaphore_signal(barrier, inc=1, device_id={axis: peer}, device_id_type=MESH)
            count += 1
    for r in range(1, rows):
        pl.semaphore_signal(barrier, inc=1, device_id={"rows": lax.rem(lax.axis_index("rows") + r, rows)}, device_id_type=MESH)
        count += 1

    load(1).start()
    pl.semaphore_wait(barrier, count)

    for p in range(len(pieces[0])):
        load(p).wait()
        if p + 2 < len(pieces[0]):
            load(p + 2).start()
        start_faces(0, p)
        start_y(0, p)
    crowd.start()
    crowd.wait()

    last = STEPS - 1
    for k in range(last):
        sent, ready = set(), 0
        for p, (lo, ny) in enumerate(pieces[k]):
            wait_recv(k, p)
            advance(k, p, ())
            ready = lo + ny
            for q, (q_lo, q_ny) in enumerate(pieces[k + 1]):
                if q not in sent and q_lo + q_ny <= ready:
                    sent.add(q)
                    start_faces(k + 1, q)
                    start_y(k + 1, q)

    zero = jnp.zeros((size_z, levels), jnp.float32)
    done = 0
    for p, (lo, ny) in enumerate(pieces[last]):
        wait_recv(last, p)
        sums = advance(last, p, (zero,) * size_x)
        means = tuple(s * (1.0 / ny) for s in sums)

        def spread(r, squares):
            deltas = [end[lo + r, tile[x], :] - means[x] for x in range(size_x)]
            return tuple(s + d * d for s, d in zip(squares, deltas))

        squares = lax.fori_loop(0, ny, spread, (zero,) * size_x)
        share = ny / (done + ny)
        for x in range(size_x):
            if done == 0:
                moments[0, 0, tile[x], :] = means[x]
                moments[0, 1, tile[x], :] = squares[x]
            else:
                delta = means[x] - moments[0, 0, tile[x], :]
                moments[0, 0, tile[x], :] += delta * share
                moments[0, 1, tile[x], :] += squares[x] + delta * delta * (done * share)
        done += ny

    for r in range(1, rows):
        moment_copy(r).start()
    wait_bytes(frecv, face_send)
    for r in range(1, rows):
        moment_copy(r).wait_recv()
    wait_bytes(fbuf.at[0, pl.ds(0, 2 * STEPS + 2 * (rows - 1))], core_send)


def finish(size_y, pieces, end, moments, standardized_hbm, end_hbm, out, end_sem, out_sem):
    rows = moments.shape[0]
    ny = size_y // pieces
    copy_end = pltpu.make_async_copy(end, end_hbm, end_sem)
    copy_end.start()

    parts = [moments[r, 0] for r in range(rows)]
    mean = sum(parts[1:], parts[0]) * (1.0 / rows)
    square = sum([moments[r, 1] for r in range(1, rows)], moments[0, 1])
    for p in parts:
        square = square + size_y * ((p - mean) * (p - mean))
    scale = lax.rsqrt(square * (1.0 / (rows * size_y)) + 0.0001)

    def store(j):
        return pltpu.make_async_copy(out.at[pl.ds(j * ny, ny)], standardized_hbm.at[pl.ds(j * ny, ny)], out_sem)

    for j in range(pieces):
        @pl.loop(0, ny)
        def _(r):
            y = j * ny + r
            out[y] = (end[y] - mean) * scale

        store(j).start()

    pltpu.make_async_copy(out, standardized_hbm, out_sem).wait()
    copy_end.wait()


def local(dims, field_values, crowding):
    shape = field_values.shape
    size_y, size_x, size_z, levels = shape
    rows, cols, slabs = dims
    counts = sorted(map(len, pieces_of(size_y)))
    arrivals = counts[0] + counts[-1]
    chunks = next(n for n in (4, 3, 6, 2, 1) if size_y % n == 0)
    flat = (size_y, size_x * size_z, levels)
    dma = pltpu.SemaphoreType.DMA
    held = (flat, (rows, 2) + flat[1:])
    out = tuple(pltpu.VMEM(each, jnp.float32) for each in held)
    vmem_spec = pl.BlockSpec(memory_space=pltpu.VMEM)
    any_spec = pl.BlockSpec(memory_space=pl.ANY)
    field_end, moments = pl.pallas_call(
        functools.partial(kernel, (rows, cols, slabs, size_y, size_x, size_z)),
        out_shape=out,
        in_specs=[any_spec] * 2,
        out_specs=(vmem_spec,) * 2,
        scratch_shapes=[
            pltpu.VMEM((STEPS, size_y + 2, size_x * size_z, levels), jnp.float32),
            pltpu.VMEM(flat, jnp.float32),
            pltpu.VMEM((STEPS, size_y, 2 * (size_z + size_x), levels), jnp.float32),
            pltpu.VMEM((STEPS, size_y, 2 * (size_z + size_x), levels), jnp.float32),
            dma((2,)),
            dma,
            dma((arrivals,)),
            dma,
            dma((2,)),
            dma((rows - 1,)),
        ],
        compiler_params=pltpu.CompilerParams(
            collective_id=0, has_side_effects=True, vmem_limit_bytes=58 * 1024 * 1024),
    )(field_values.reshape(flat), crowding.reshape(flat))
    whole = jax.ShapeDtypeStruct(flat, jnp.float32)
    standardized, field_end = pl.pallas_call(
        functools.partial(finish, size_y, chunks),
        out_shape=(whole, whole),
        in_specs=[vmem_spec] * 2,
        out_specs=(any_spec,) * 2,
        scratch_shapes=[pltpu.VMEM(flat, jnp.float32), dma, dma],
        compiler_params=pltpu.CompilerParams(vmem_limit_bytes=16 * 1024 * 1024),
    )(*(pltpu.with_memory_space_constraint(each, pltpu.VMEM) for each in (field_end, moments)))
    return standardized.reshape(shape), field_end.reshape(shape)


def solution(mesh):
    spec = P(("site", "rows"), "cols", "slabs", None)
    dims = tuple(mesh.shape[axis] for axis in ("rows", "cols", "slabs"))
    return jax.shard_map(
        functools.partial(local, dims), mesh=mesh,
        in_specs=(spec, spec), out_specs=(spec, spec), check_vma=False)
```

```python
import functools

import jax
import jax.numpy as jnp
from jax import lax
from jax.experimental import pallas as pl
from jax.experimental.pallas import tpu as pltpu
from jax.sharding import PartitionSpec as P

MESH = pl.DeviceIdType.MESH
STEPS = 6


def ring(axis, devices):
    me = lax.axis_index(axis)
    return lax.rem(me + 1, devices), lax.rem(me + devices - 1, devices)


def pieces_of(size_y):
    def cut(*parts):
        ends = sorted({size_y * part // 24 for part in parts} | {0, size_y})
        return tuple((lo, hi - lo) for lo, hi in zip(ends, ends[1:]))

    return (cut(2, 8, 16),) + (cut(8, 16),) * (STEPS - 2) + (cut(10, 17, 21, 23),)


def kernel(dims, f_hbm, c_hbm, end, moments, fbuf, cbuf, fsend, frecv,
           load_sem, face_send, face_recv, core_send, row_recv):
    rows, cols, slabs, size_y, size_x, size_z = dims
    pieces = pieces_of(size_y)
    common = min(map(len, pieces))
    levels = f_hbm.shape[-1]
    x_next = ring("cols", cols)
    z_next = ring("slabs", slabs)
    x_copies = 1 if cols == 2 else 2
    y_next = ring("rows", rows)
    tile = [pl.ds(x * size_z, size_z) for x in range(size_x)]

    x_part = [pl.ds(side * size_z, size_z) for side in (0, 1)]
    z_first = [2 * size_z + side * size_x for side in (0, 1)]
    z_part = [pl.ds(first, size_x) for first in z_first]

    def arrived(k, p):
        return (k % 2) * common + p if p < common else 2 * common + p - common

    def faces(k, p):
        copies = []
        at_rows = pl.ds(*pieces[k][p])
        for axis, devices, parts, whole, peers in (
                ("cols", cols, x_part, pl.ds(0, 2 * size_z), x_next),
                ("slabs", slabs, z_part, pl.ds(2 * size_z, 2 * size_x), z_next)):
            for side in range(1 if devices == 2 else 2):
                part = whole if devices == 2 else parts[side]
                copies.append(pltpu.make_async_remote_copy(
                    src_ref=fsend.at[k, at_rows, part], dst_ref=frecv.at[k, at_rows, part],
                    send_sem=face_send, recv_sem=face_recv.at[arrived(k, p)],
                    device_id={axis: peers[side]}, device_id_type=MESH))
        return copies

    def y_copy(k, side):
        return pltpu.make_async_remote_copy(
            src_ref=fbuf.at[k, size_y if side == 0 else 1],
            dst_ref=fbuf.at[k, 0 if side == 0 else size_y + 1],
            send_sem=core_send, recv_sem=row_recv.at[k % 2],
            device_id={"rows": y_next[side]}, device_id_type=MESH)

    def wait_bytes(ref, sem):
        pltpu.make_async_copy(ref, ref, sem).wait()

    def load(p):
        lo, ny = pieces[0][p]
        return pltpu.make_async_copy(f_hbm.at[pl.ds(lo, ny)], fbuf.at[0, pl.ds(lo + 1, ny)], load_sem.at[p % 2])

    crowd = pltpu.make_async_copy(c_hbm, cbuf, load_sem.at[0])

    def start_faces(k, p):
        lo, ny = pieces[k][p]
        copies = faces(k, p)
        if k:
            for copy in copies[:x_copies]:
                copy.start()

        @pl.loop(0, ny)
        def _(r):
            y = lo + r
            for side in (0, 1):
                first = size_z - 1 if side == 0 else 0
                fsend[k, y, z_part[side]] = fbuf[k, y + 1, pl.ds(first, size_x, stride=size_z), :]
                if not k:
                    fsend[k, y, x_part[side]] = fbuf[k, y + 1, tile[size_x - 1 if side == 0 else 0], :]

        for copy in copies[x_copies if k else 0:]:
            copy.start()

    def start_y(k, p):
        lo, ny = pieces[k][p]
        if lo == 0:
            y_copy(k, 1).start()
        if lo + ny == size_y:
            y_copy(k, 0).start()

    def wait_recv(k, p):
        lo, ny = pieces[k][p]
        wait_bytes(frecv.at[k, pl.ds(lo, ny)], face_recv.at[arrived(k, p)])
        if p == 0:
            wait_bytes(fbuf.at[k, pl.ds(0, 2)], row_recv.at[k % 2])

    at_z = lax.broadcasted_iota(jnp.int32, (size_z, levels), 0)

    def advance(k, p, sums):
        lo, ny = pieces[k][p]

        def row(r, sums):
            y = lo + r
            mid = [fbuf[k, y + 1, tile[x], :] for x in range(size_x)]
            out = []
            for x in range(size_x):
                m = mid[x]
                below = mid[x - 1] if x > 0 else frecv[k, y, x_part[0]]
                above = mid[x + 1] if x < size_x - 1 else frecv[k, y, x_part[1]]
                z_lo = jnp.broadcast_to(frecv[k, y, pl.ds(z_first[0] + x, 1), :], m.shape)
                z_hi = jnp.broadcast_to(frecv[k, y, pl.ds(z_first[1] + x, 1), :], m.shape)
                left = jnp.where(at_z == 0, z_lo, pltpu.roll(m, 1, 0))
                right = jnp.where(at_z == size_z - 1, z_hi, pltpu.roll(m, size_z - 1, 0))
                near = (fbuf[k, y, tile[x], :] + fbuf[k, y + 2, tile[x], :]) + (below + above) + (left + right)
                new = 0.1 * near + m * (0.6 - 0.2 * (m * cbuf[y, tile[x], :]))
                if sums:
                    end[y, tile[x], :] = new
                else:
                    fbuf[k + 1, y + 1, tile[x], :] = new
                    if x == size_x - 1:
                        fsend[k + 1, y, x_part[0]] = new
                    if x == 0:
                        fsend[k + 1, y, x_part[1]] = new
                out.append(new)
            return tuple(s + o for s, o in zip(sums, out)) if sums else ()

        return lax.fori_loop(0, ny, row, sums)

    load(0).start()

    barrier = pltpu.get_barrier_semaphore()
    count = 0
    for axis, devices, peers in (("cols", cols, x_next), ("slabs", slabs, z_next)):
        for peer in peers[:1 if devices == 2 else 2]:
            pl.semaphore_signal(barrier, inc=1, device_id={axis: peer}, device_id_type=MESH)
            count += 1
    for r in range(1, rows):
        pl.semaphore_signal(barrier, inc=1, device_id={"rows": lax.rem(lax.axis_index("rows") + r, rows)}, device_id_type=MESH)
        count += 1

    load(1).start()
    pl.semaphore_wait(barrier, count)

    for p in range(len(pieces[0])):
        load(p).wait()
        if p + 2 < len(pieces[0]):
            load(p + 2).start()
        start_faces(0, p)
        start_y(0, p)
    crowd.start()
    crowd.wait()

    last = STEPS - 1
    for k in range(last):
        sent, ready = set(), 0
        for p, (lo, ny) in enumerate(pieces[k]):
            wait_recv(k, p)
            advance(k, p, ())
            ready = lo + ny
            for q, (q_lo, q_ny) in enumerate(pieces[k + 1]):
                if q not in sent and q_lo + q_ny <= ready:
                    sent.add(q)
                    start_faces(k + 1, q)
                    start_y(k + 1, q)

    zero = jnp.zeros((size_z, levels), jnp.float32)
    done = 0
    for p, (lo, ny) in enumerate(pieces[last]):
        wait_recv(last, p)
        sums = advance(last, p, (zero,) * size_x)
        means = tuple(s * (1.0 / ny) for s in sums)

        def spread(r, squares):
            deltas = [end[lo + r, tile[x], :] - means[x] for x in range(size_x)]
            return tuple(s + d * d for s, d in zip(squares, deltas))

        squares = lax.fori_loop(0, ny, spread, (zero,) * size_x)
        share = ny / (done + ny)
        for x in range(size_x):
            if done == 0:
                moments[0, tile[x], :] = means[x]
                moments[1, tile[x], :] = squares[x]
            else:
                delta = means[x] - moments[0, tile[x], :]
                moments[0, tile[x], :] += delta * share
                moments[1, tile[x], :] += squares[x] + delta * delta * (done * share)
        done += ny

    wait_bytes(frecv, face_send)
    wait_bytes(fbuf.at[0, pl.ds(0, 2 * STEPS)], core_send)


def keep(head, end, end_hbm, end_sem):
    at = pl.ds(0, head)
    copy_end = pltpu.make_async_copy(end.at[at], end_hbm.at[at], end_sem)
    copy_end.start()
    copy_end.wait()


def finish(size_y, head, pieces, kept_hbm, end, *refs):
    moments, (standardized_hbm, end_hbm, out, out_sem, end_sem) = refs[:-5], refs[-5:]
    rows = len(moments)
    at = pl.ds(head, size_y - head)
    copy_end = pltpu.make_async_copy(end.at[at], end_hbm.at[at], end_sem)
    copy_end.start()
    ny = size_y // pieces
    parts = [m[0] for m in moments]
    mean = sum(parts[1:], parts[0]) * (1.0 / rows)
    square = sum([m[1] for m in moments[1:]], moments[0][1])
    for p in parts:
        square = square + size_y * ((p - mean) * (p - mean))
    scale = lax.rsqrt(square * (1.0 / (rows * size_y)) + 0.0001)

    for j in range(pieces):
        @pl.loop(0, ny)
        def _(r):
            y = j * ny + r
            out[y] = (end[y] - mean) * scale

        at = pl.ds(j * ny, ny)
        pltpu.make_async_copy(out.at[at], standardized_hbm.at[at], out_sem).start()
    pltpu.make_async_copy(out, standardized_hbm, out_sem).wait()
    copy_end.wait()


def local(dims, field_values, crowding):
    shape = field_values.shape
    size_y, size_x, size_z, levels = shape
    rows, cols, slabs = dims
    counts = sorted(map(len, pieces_of(size_y)))
    arrivals = counts[0] + counts[-1]
    chunks = next(n for n in (4, 3, 6, 2, 1) if size_y % n == 0)
    flat = (size_y, size_x * size_z, levels)
    dma = pltpu.SemaphoreType.DMA
    held = (flat, (2,) + flat[1:])
    out = tuple(pltpu.VMEM(each, jnp.float32) for each in held)
    vmem_spec = pl.BlockSpec(memory_space=pltpu.VMEM)
    any_spec = pl.BlockSpec(memory_space=pl.ANY)
    field_end, moments = pl.pallas_call(
        functools.partial(kernel, (rows, cols, slabs, size_y, size_x, size_z)),
        out_shape=out,
        in_specs=[any_spec] * 2,
        out_specs=(vmem_spec,) * 2,
        scratch_shapes=[
            pltpu.VMEM((STEPS, size_y + 2, size_x * size_z, levels), jnp.float32),
            pltpu.VMEM(flat, jnp.float32),
            pltpu.VMEM((STEPS, size_y, 2 * (size_z + size_x), levels), jnp.float32),
            pltpu.VMEM((STEPS, size_y, 2 * (size_z + size_x), levels), jnp.float32),
            dma((2,)),
            dma,
            dma((arrivals,)),
            dma,
            dma((2,)),
        ],
        compiler_params=pltpu.CompilerParams(
            collective_id=0, has_side_effects=True, vmem_limit_bytes=58 * 1024 * 1024),
    )(field_values.reshape(flat), crowding.reshape(flat))
    def held_in_vmem(each):
        return pltpu.with_memory_space_constraint(each, pltpu.VMEM)

    whole = jax.ShapeDtypeStruct(flat, jnp.float32)
    head = size_y * 5 // 8
    small = pltpu.CompilerParams(vmem_limit_bytes=16 * 1024 * 1024)
    others = [lax.ppermute(moments, "rows", [(i, (i + r) % rows) for i in range(rows)]) for r in range(1, rows)]
    field_in_vmem = held_in_vmem(field_end)
    kept = pl.pallas_call(
        functools.partial(keep, head), out_shape=whole, in_specs=[vmem_spec], out_specs=any_spec, scratch_shapes=[dma], compiler_params=small,
        cost_estimate=pl.CostEstimate(flops=2 * 10 ** 8, bytes_accessed=0, transcendentals=0),
    )(field_in_vmem)
    standardized, field_end = pl.pallas_call(
        functools.partial(finish, size_y, head, chunks),
        out_shape=(whole, whole),
        in_specs=[any_spec] + [vmem_spec] * (1 + rows),
        out_specs=(any_spec,) * 2,
        scratch_shapes=[pltpu.VMEM(flat, jnp.float32), dma, dma],
        input_output_aliases={0: 1},
        compiler_params=small,
    )(kept, field_in_vmem, held_in_vmem(moments), *others)
    return standardized.reshape(shape), field_end.reshape(shape)


def solution(mesh):
    spec = P(("site", "rows"), "cols", "slabs", None)
    dims = tuple(mesh.shape[axis] for axis in ("rows", "cols", "slabs"))
    return jax.shard_map(
        functools.partial(local, dims), mesh=mesh,
        in_specs=(spec, spec), out_specs=(spec, spec), check_vma=False)
```
